32 devices in a mesh: vocab: 16 (over z, y, x), dp: 2 (over core).
Axes of the slice: x: 2, y: 2, z: 4, core: 2. Of those that a mesh axis runs over, the one named last changes fastest.
Arguments:
- embed_table: bfloat16 [16384, 4096], P('vocab'), may hold values from -3 to 3
- token_ids: int32 [2, 16384], P('dp', 'vocab'), may hold values from 0 to 16383, as said below
- grad_rows: bfloat16 [2, 16384, 4096], P('dp', 'vocab'), may hold values from -12 to 12
Outputs:
- updated: bfloat16 [16384, 4096], P('vocab', 'dp')
- grad_rms: float32 [1], replicated
The draws below stay inside these ranges and needn't reach their ends.
Inputs may be any that keep to these rules, and one draw needn't show every extreme that they name: `token_ids`: rows are read cyclically: row r stands for every r + k * 16384. The window of vocab index v (tokens v * 1024 to (v + 1) * 1024 - 1 of a replica) holds ids that, read as the cyclic representatives from v * 1024 - 256 to (v + 1) * 1024 + 255, rise (never fall) along its tokens; both ends are reached in some window. Only its first 128 and last 128 tokens may lie outside rows v * 1024 to (v + 1) * 1024 - 1 (so read), the first ones below, the last ones above; in every window its first token lies below and its last above, in some window all first 128 lie below, in some all last 128 above.
All inputs are finite; a program needn't handle non-finite values.
Results may differ from the reference program's by a relative error of at most 0.002.
Values may be sent and summed in bfloat16 or wider, within the bound.
A program may use at most 128 MiB of HBM per device.

```python
import jax
import jax.numpy as jnp

D = 4096
ROWS_DEV = 1024
EDGE = 256
TOK_EDGE = 128
TOK_DEV = 1024
VOCAB = 16384
TOKENS = 16384
N_DP = 2


def draw_replica(key):
    windows = TOKENS // TOK_DEV
    key_above, key_below, key_first, key_middle, key_last = jax.random.split(key, 5)
    below = jax.random.randint(key_below, (windows,), 1, EDGE + 1)
    below = below.at[1].set(EDGE)
    above = jax.random.randint(key_above, (windows,), 1, EDGE + 1)
    above = above.at[windows - 1].set(EDGE)
    reach_up = jnp.roll(above, -1)
    device_ids = jnp.arange(windows, dtype=jnp.int32)
    starts = device_ids * ROWS_DEV
    first_low = starts - below
    first_high = jnp.where(device_ids == 1, starts, starts + ROWS_DEV // 2)
    last_low = jnp.where(device_ids == windows - 2, starts + ROWS_DEV, starts + ROWS_DEV - ROWS_DEV // 2)
    last_high = starts + ROWS_DEV + reach_up
    first_group = jax.random.randint(key_first, (windows, TOK_EDGE), first_low[:, None], first_high[:, None])
    first_group = first_group.at[:, 0].set(first_low)
    middle_group = jax.random.randint(key_middle, (windows, TOK_DEV - 2 * TOK_EDGE), starts[:, None], starts[:, None] + ROWS_DEV)
    last_group = jax.random.randint(key_last, (windows, TOK_EDGE), last_low[:, None], last_high[:, None])
    last_group = last_group.at[:, TOK_EDGE - 1].set(last_high - 1)
    window_ids = jnp.sort(jnp.concatenate([first_group, middle_group, last_group], axis=1), axis=1)
    window_ids = jnp.mod(window_ids, windows * ROWS_DEV)
    return window_ids.reshape(windows * TOK_DEV).astype(jnp.int32)


def draw_token_ids(key, part):
    replica_keys = jax.random.split(jax.random.fold_in(key, 11), N_DP)
    return jnp.stack([draw_replica(replica_keys[index]) for index in range(N_DP)])


def draw_grad_rows(key, part):
    windows = TOKENS // TOK_DEV
    key_base = jax.random.fold_in(jax.random.fold_in(key, 23), 0)
    key_window = jax.random.fold_in(jax.random.fold_in(key, 23), 3)
    values = jax.random.normal(key_base, (N_DP, TOKENS, D), jnp.float32)
    window_scale = jnp.exp(jax.random.uniform(key_window, (N_DP, windows, 1), jnp.float32, -1.2, 1.2))
    window_scale = jnp.repeat(window_scale, TOK_DEV, axis=1)
    values = window_scale * values
    return jnp.clip(values, -12.0, 12.0).astype(jnp.bfloat16)


def block_levels(own_key, extent, shards, least, high):
    gain = 1.0
    for axis_at, blocks in shards:
        steps = jax.random.uniform(jax.random.fold_in(jax.random.fold_in(own_key, 6), axis_at), (blocks,), jnp.float32, least / len(shards), high / len(shards))
        gain = gain * jnp.repeat(jnp.exp(steps), extent[axis_at] // blocks).reshape((-1,) + (1,) * (len(extent) - 1 - axis_at))
    return gain


def centred(own_key, shape, width, limit, cuts=(), kind=jnp.bfloat16):
    entries = width * jax.random.normal(own_key, shape, jnp.float32)
    if cuts:
        entries = entries * block_levels(own_key, shape, cuts, -0.22, 0.18)
    return jnp.clip(entries, -limit, limit).astype(kind)


def setup_inputs(seed: int = 0) -> dict:
    streams_of = jax.random.split(jax.random.key(seed), 4)
    embed_table = centred(streams_of[0], (VOCAB, D), 0.5, 3.0, ((0, 16),))
    token_ids = draw_token_ids(jax.random.fold_in(streams_of[3], 71), 0)
    grad_rows = draw_grad_rows(jax.random.fold_in(streams_of[3], 71), 0)
    return {"embed_table": embed_table, "token_ids": token_ids, "grad_rows": grad_rows}


step_rate = 0.5
norm_limit = 1.0

def reference(embed_table, token_ids, grad_rows):
    gradient = jnp.zeros((VOCAB, D), jnp.float32)
    for replica in range(N_DP):
        gradient = gradient + jax.ops.segment_sum(grad_rows[replica].astype(jnp.float32), token_ids[replica], num_segments=VOCAB)
    grad_rms = jnp.sqrt(jnp.sum(gradient * gradient) / (VOCAB * D))
    clip_scale = 1.0 / jnp.maximum(1.0, grad_rms / norm_limit)
    updated = (embed_table.astype(jnp.float32) - step_rate * clip_scale * gradient).astype(jnp.bfloat16)
    return (updated, jnp.reshape(grad_rms, (1,)))
```

```python
import functools

import jax
import jax.numpy as jnp
from jax import lax
from jax.experimental import pallas as pl
from jax.experimental.pallas import tpu as pltpu
from jax.sharding import PartitionSpec as P

MESH = pl.DeviceIdType.MESH
TOK_EDGE = 128
EDGE = 256
COLS = 512
STORE_ROWS = 128

step_rate = 0.5
norm_limit = 1.0


def kernel(sizes, table_ref, ids_ref, grad_ref, out_ref, rms_ref,
           toks, halo, table, grad, outbuf, mate_ids, halo_ids, square, sums,
           own_sem, table_sem, mate_sem, mate_id_sem, halo_send, halo_recv,
           halo_id_send, halo_id_recv, sum_send, sum_recv, out_sem):
    n_vocab, n_dp = sizes
    rows, width = table_ref.shape
    tokens = ids_ref.shape[1]
    half = width // n_dp
    n = n_vocab * n_dp
    chunks = half // COLS
    blocks = rows // EDGE
    v = lax.axis_index("vocab")
    p = lax.axis_index("dp")
    me = v * n_dp + p
    mate = 1 - p
    below = lax.rem(v + n_vocab - 1, n_vocab)
    above = lax.rem(v + 1, n_vocab)

    def columns(core, chunk):
        return pl.ds(pl.multiple_of(core * half + chunk * COLS, COLS), COLS)

    def place(index):
        return {"vocab": lax.div(index, n_dp), "dp": lax.rem(index, n_dp)}

    own_half = pl.ds(pl.multiple_of(p * half, half), half)
    own_copy = pltpu.make_async_copy(
        grad_ref.at[0, :, own_half], toks.at[pl.ds(0, tokens), :], own_sem
    )
    own_copy.start()
    table_copy = pltpu.make_async_copy(table_ref.at[:, own_half], table, table_sem)

    barrier = pltpu.get_barrier_semaphore()

    @pl.loop(1, n)
    def _(i):
        pl.semaphore_signal(
            barrier, inc=1, device_id=place(lax.rem(me + i, n)), device_id_type=MESH
        )

    pl.semaphore_wait(barrier, n - 1)

    def remote(src, dst, send, recv, device):
        return pltpu.make_async_remote_copy(
            src_ref=src, dst_ref=dst, send_sem=send, recv_sem=recv,
            device_id=device, device_id_type=MESH,
        )

    sent = []
    mate_id_copy = remote(
        ids_ref, mate_ids, mate_id_sem.at[0], mate_id_sem.at[1], {"vocab": v, "dp": mate}
    )
    mate_id_copy.start()
    sides = ((0, 0, below), (1, tokens - TOK_EDGE, above))
    for side, first, target in sides:
        for core in range(n_dp):
            copy = remote(
                ids_ref.at[:, pl.ds(first, TOK_EDGE)], halo_ids.at[side, p],
                halo_id_send.at[side, core], halo_id_recv.at[side, p],
                {"vocab": target, "dp": core},
            )
            copy.start()
            sent.append(copy)
    mate_copies = []
    for chunk in range(chunks):
        for side, first, target in sides:
            for core in range(n_dp):
                copy = remote(
                    grad_ref.at[0, pl.ds(first, TOK_EDGE), columns(core, chunk)],
                    halo.at[side, p, :, pl.ds(chunk * COLS, COLS)],
                    halo_send.at[side, core, chunk], halo_recv.at[side, p, chunk],
                    {"vocab": target, "dp": core},
                )
                copy.start()
                sent.append(copy)
        copy = remote(
            grad_ref.at[0, :, columns(mate, chunk)],
            toks.at[pl.ds(tokens, tokens), pl.ds(chunk * COLS, COLS)],
            mate_sem.at[0, chunk], mate_sem.at[1, chunk], {"vocab": v, "dp": mate},
        )
        copy.start()
        mate_copies.append(copy)
    table_copy.start()

    own_start = v * rows

    def local(ids):
        shifted = ids - own_start
        return jnp.where(shifted < 0, shifted + n_vocab * rows, shifted)

    def onehot(ids, base, count):
        index = lax.broadcasted_iota(jnp.int32, (count, ids.shape[1]), 0) + base
        return jnp.where(ids == index, 1.0, 0.0).astype(jnp.bfloat16)

    def add_squares(values):
        lanes = values * values
        lanes = jnp.sum(lanes.reshape(EDGE // 8, 8, COLS), axis=0)
        square[...] += lanes

    square[...] = jnp.zeros_like(square)
    own_copy.wait()
    mate_id_copy.wait()
    for copy in mate_copies:
        copy.wait()
    window_ids = local(jnp.concatenate([ids_ref[...], mate_ids[...]], axis=1))
    for block in range(blocks):
        picked = onehot(window_ids, block * EDGE, EDGE)

        @pl.loop(0, chunks)
        def _(chunk):
            here = pl.ds(pl.multiple_of(chunk * COLS, COLS), COLS)
            part = jnp.dot(picked, toks[:, here], preferred_element_type=jnp.float32)
            grad[pl.ds(block * EDGE, EDGE), here] = part
            if 0 < block < blocks - 1:
                add_squares(part)

    table_copy.wait()
    halo_pick = []
    for side in range(2):
        for core in range(n_dp):
            remote(
                ids_ref.at[:, pl.ds(0, TOK_EDGE)], halo_ids.at[side, core],
                halo_id_send.at[side, core], halo_id_recv.at[side, core],
                {"vocab": above, "dp": core},
            ).wait_recv()
        ids = local(jnp.concatenate([halo_ids[side, core] for core in range(n_dp)], axis=1))
        base = (rows - EDGE) if side == 0 else 0
        halo_pick.append((base, onehot(ids, base, EDGE)))
    for chunk in range(chunks):
        here = pl.ds(chunk * COLS, COLS)
        for side in range(2):
            for core in range(n_dp):
                remote(
                    grad_ref.at[0, pl.ds(0, TOK_EDGE), pl.ds(0, COLS)],
                    halo.at[side, core, :, here],
                    halo_send.at[side, core, chunk], halo_recv.at[side, core, chunk],
                    {"vocab": above, "dp": core},
                ).wait_recv()
            base, pick = halo_pick[side]
            part = jnp.dot(
                pick, halo[side, :, :, here].reshape(n_dp * TOK_EDGE, COLS),
                preferred_element_type=jnp.float32,
            )
            total = grad[pl.ds(base, EDGE), here] + part
            grad[pl.ds(base, EDGE), here] = total
            add_squares(total)

    lanes = jnp.sum(square[...], axis=0, keepdims=True)
    lanes = functools.reduce(
        jnp.add, [lanes[:, k * 128:(k + 1) * 128] for k in range(COLS // 128)]
    )
    sums[me] = lanes

    def sum_copy(i, source, target):
        return remote(
            sums.at[source], sums.at[source], sum_send.at[i], sum_recv.at[source], place(target)
        )

    @pl.loop(1, n)
    def _(i):
        sum_copy(i, me, lax.rem(me + i, n)).start()

    for copy in sent:
        copy.wait_send()

    @pl.loop(1, n)
    def _(i):
        source = lax.rem(me + i, n)
        sum_copy(i, source, source).wait_recv()

    total = jnp.sum(jnp.sum(sums[...], axis=0), axis=1, keepdims=True)
    rms = jnp.sqrt(total / (n_vocab * rows * width))
    clip_scale = 1.0 / jnp.maximum(1.0, rms / norm_limit)
    rms_ref[0] = rms[0, 0]
    rate = step_rate * clip_scale

    stores = []
    for block in range(rows // STORE_ROWS):
        here = pl.ds(block * STORE_ROWS, STORE_ROWS)
        moved = table[here, :].astype(jnp.float32) - rate * grad[here, :]
        outbuf[here, :] = moved.astype(jnp.bfloat16)
        copy = pltpu.make_async_copy(outbuf.at[here, :], out_ref.at[here, :], out_sem.at[block])
        copy.start()
        stores.append(copy)

    @pl.loop(1, n)
    def _(i):
        sum_copy(i, me, lax.rem(me + i, n)).wait_send()

    for copy in stores:
        copy.wait()


def solution(mesh):
    n_vocab, n_dp = mesh.shape["vocab"], mesh.shape["dp"]
    n = n_vocab * n_dp

    def body(embed_table, token_ids, grad_rows):
        rows, width = embed_table.shape
        tokens = token_ids.shape[1]
        half = width // n_dp
        chunks = half // COLS
        anywhere = pl.BlockSpec(memory_space=pl.ANY)
        updated, grad_rms = pl.pallas_call(
            functools.partial(kernel, (n_vocab, n_dp)),
            name="clipped_update",
            out_shape=(
                jax.ShapeDtypeStruct((rows, half), jnp.bfloat16),
                jax.ShapeDtypeStruct((1,), jnp.float32),
            ),
            in_specs=[anywhere, pl.BlockSpec(memory_space=pltpu.VMEM), anywhere],
            out_specs=(anywhere, pl.BlockSpec(memory_space=pltpu.SMEM)),
            scratch_shapes=[
                pltpu.VMEM((n_dp * tokens, half), jnp.bfloat16),
                pltpu.VMEM((2, n_dp, TOK_EDGE, half), jnp.bfloat16),
                pltpu.VMEM((rows, half), jnp.bfloat16),
                pltpu.VMEM((rows, half), jnp.float32),
                pltpu.VMEM((rows, half), jnp.bfloat16),
                pltpu.VMEM((1, tokens), jnp.int32),
                pltpu.VMEM((2, n_dp, 1, TOK_EDGE), jnp.int32),
                pltpu.VMEM((8, COLS), jnp.float32),
                pltpu.VMEM((n, 1, 128), jnp.float32),
                pltpu.SemaphoreType.DMA,
                pltpu.SemaphoreType.DMA,
                pltpu.SemaphoreType.DMA((2, chunks)),
                pltpu.SemaphoreType.DMA((2,)),
                pltpu.SemaphoreType.DMA((2, n_dp, chunks)),
                pltpu.SemaphoreType.DMA((2, n_dp, chunks)),
                pltpu.SemaphoreType.DMA((2, n_dp)),
                pltpu.SemaphoreType.DMA((2, n_dp)),
                pltpu.SemaphoreType.DMA((n,)),
                pltpu.SemaphoreType.DMA((n,)),
                pltpu.SemaphoreType.DMA((rows // STORE_ROWS,)),
            ],
            compiler_params=pltpu.CompilerParams(
                collective_id=0, has_side_effects=True, vmem_limit_bytes=60 * 1024 * 1024
            ),
        )(embed_table, token_ids, grad_rows)
        return updated, grad_rms

    in_specs = (P("vocab", None), P("dp", "vocab"), P("dp", "vocab", None))
    out_specs = (P("vocab", "dp"), P())
    return jax.shard_map(body, mesh=mesh, in_specs=in_specs, out_specs=out_specs, check_vma=False)
```

```python
import functools

import jax
import jax.numpy as jnp
from jax import lax
from jax.experimental import pallas as pl
from jax.experimental.pallas import tpu as pltpu
from jax.sharding import PartitionSpec as P

MESH = pl.DeviceIdType.MESH
TOK_EDGE = 128
EDGE = 256
COLS = 512
STORE_ROWS = 128

step_rate = 0.5
norm_limit = 1.0


def kernel(sizes, table_ref, ids_ref, grad_ref, grad, table, norm_ref,
           toks, halo, own_ids, mate_ids, halo_ids, square, sums,
           own_sem, own_id_sem, table_sem, mate_sem, mate_id_sem, halo_send, halo_recv,
           halo_id_send, halo_id_recv, sum_send, sum_recv):
    n_vocab, n_dp = sizes
    rows, width = table_ref.shape
    tokens = ids_ref.shape[1]
    half = width // n_dp
    n = n_vocab * n_dp
    chunks = half // COLS
    blocks = rows // EDGE
    v = lax.axis_index("vocab")
    p = lax.axis_index("dp")
    me = v * n_dp + p
    mate = 1 - p
    below = lax.rem(v + n_vocab - 1, n_vocab)
    above = lax.rem(v + 1, n_vocab)

    def columns(core, chunk):
        return pl.ds(pl.multiple_of(core * half + chunk * COLS, COLS), COLS)

    def place(index):
        return {"vocab": lax.div(index, n_dp), "dp": lax.rem(index, n_dp)}

    own_half = pl.ds(pl.multiple_of(p * half, half), half)
    own_copy = pltpu.make_async_copy(
        grad_ref.at[0, :, own_half], toks.at[pl.ds(0, tokens), :], own_sem
    )
    own_copy.start()
    own_id_copy = pltpu.make_async_copy(ids_ref, own_ids, own_id_sem)
    own_id_copy.start()
    table_copy = pltpu.make_async_copy(table_ref.at[:, own_half], table, table_sem)

    barrier = pltpu.get_barrier_semaphore()

    @pl.loop(1, n)
    def _(i):
        pl.semaphore_signal(
            barrier, inc=1, device_id=place(lax.rem(me + i, n)), device_id_type=MESH
        )

    pl.semaphore_wait(barrier, n - 1)

    def remote(src, dst, send, recv, device):
        return pltpu.make_async_remote_copy(
            src_ref=src, dst_ref=dst, send_sem=send, recv_sem=recv,
            device_id=device, device_id_type=MESH,
        )

    sent = []
    mate_id_copy = remote(
        ids_ref, mate_ids, mate_id_sem.at[0], mate_id_sem.at[1], {"vocab": v, "dp": mate}
    )
    mate_id_copy.start()
    sides = ((0, 0, below), (1, tokens - TOK_EDGE, above))
    for side, first, target in sides:
        for core in range(n_dp):
            copy = remote(
                ids_ref.at[:, pl.ds(first, TOK_EDGE)], halo_ids.at[side, p],
                halo_id_send.at[side, core], halo_id_recv.at[side, p],
                {"vocab": target, "dp": core},
            )
            copy.start()
            sent.append(copy)
    mate_copies = []
    for chunk in range(chunks):
        for side, first, target in sides:
            for core in range(n_dp):
                copy = remote(
                    grad_ref.at[0, pl.ds(first, TOK_EDGE), columns(core, chunk)],
                    halo.at[side, p, :, pl.ds(chunk * COLS, COLS)],
                    halo_send.at[side, core, chunk], halo_recv.at[side, p, chunk],
                    {"vocab": target, "dp": core},
                )
                copy.start()
                sent.append(copy)
        copy = remote(
            grad_ref.at[0, :, columns(mate, chunk)],
            toks.at[pl.ds(tokens, tokens), pl.ds(chunk * COLS, COLS)],
            mate_sem.at[0, chunk], mate_sem.at[1, chunk], {"vocab": v, "dp": mate},
        )
        copy.start()
        mate_copies.append(copy)
    table_copy.start()

    own_start = v * rows

    def local(ids):
        shifted = ids - own_start
        return jnp.where(shifted < 0, shifted + n_vocab * rows, shifted)

    def onehot(ids, base, count):
        index = lax.broadcasted_iota(jnp.int32, (count, ids.shape[1]), 0) + base
        return jnp.where(ids == index, 1.0, 0.0).astype(jnp.bfloat16)

    def add_squares(values):
        lanes = values * values
        lanes = jnp.sum(lanes.reshape(EDGE // 8, 8, COLS), axis=0)
        square[...] += lanes

    square[...] = jnp.zeros_like(square)
    own_copy.wait()
    own_id_copy.wait()
    mate_id_copy.wait()
    for copy in mate_copies:
        copy.wait()
    window_ids = local(jnp.concatenate([own_ids[...], mate_ids[...]], axis=1))
    for block in range(blocks):
        picked = onehot(window_ids, block * EDGE, EDGE)

        @pl.loop(0, chunks)
        def _(chunk):
            here = pl.ds(pl.multiple_of(chunk * COLS, COLS), COLS)
            part = jnp.dot(picked, toks[:, here], preferred_element_type=jnp.float32)
            grad[pl.ds(block * EDGE, EDGE), here] = part
            if 0 < block < blocks - 1:
                add_squares(part)

    table_copy.wait()
    halo_pick = []
    for side in range(2):
        for core in range(n_dp):
            remote(
                ids_ref.at[:, pl.ds(0, TOK_EDGE)], halo_ids.at[side, core],
                halo_id_send.at[side, core], halo_id_recv.at[side, core],
                {"vocab": above, "dp": core},
            ).wait_recv()
        ids = local(jnp.concatenate([halo_ids[side, core] for core in range(n_dp)], axis=1))
        base = (rows - EDGE) if side == 0 else 0
        halo_pick.append((base, onehot(ids, base, EDGE)))
    for chunk in range(chunks):
        here = pl.ds(chunk * COLS, COLS)
        for side in range(2):
            for core in range(n_dp):
                remote(
                    grad_ref.at[0, pl.ds(0, TOK_EDGE), pl.ds(0, COLS)],
                    halo.at[side, core, :, here],
                    halo_send.at[side, core, chunk], halo_recv.at[side, core, chunk],
                    {"vocab": above, "dp": core},
                ).wait_recv()
            base, pick = halo_pick[side]
            part = jnp.dot(
                pick, halo[side, :, :, here].reshape(n_dp * TOK_EDGE, COLS),
                preferred_element_type=jnp.float32,
            )
            total = grad[pl.ds(base, EDGE), here] + part
            grad[pl.ds(base, EDGE), here] = total
            add_squares(total)

    lanes = jnp.sum(square[...], axis=0, keepdims=True)
    lanes = functools.reduce(
        jnp.add, [lanes[:, k * 128:(k + 1) * 128] for k in range(COLS // 128)]
    )
    sums[me] = lanes

    def sum_copy(i, source, target):
        return remote(
            sums.at[source], sums.at[source], sum_send.at[i], sum_recv.at[source], place(target)
        )

    @pl.loop(1, n)
    def _(i):
        sum_copy(i, me, lax.rem(me + i, n)).start()

    for copy in sent:
        copy.wait_send()

    @pl.loop(1, n)
    def _(i):
        source = lax.rem(me + i, n)
        sum_copy(i, source, source).wait_recv()

    total = jnp.sum(jnp.sum(sums[...], axis=0), axis=1, keepdims=True)
    rms = jnp.sqrt(total / (n_vocab * rows * width))
    clip_scale = 1.0 / jnp.maximum(1.0, rms / norm_limit)
    norm_ref[0:1, :] = jnp.broadcast_to(step_rate * clip_scale, (1, 128))
    norm_ref[1:2, :] = jnp.broadcast_to(rms, (1, 128))

    @pl.loop(1, n)
    def _(i):
        sum_copy(i, me, lax.rem(me + i, n)).wait_send()


def update(grad, table, norm_ref, out_ref, rms_ref, outbuf, out_sem):
    rate = norm_ref[0:1, 0:1]
    stores = []
    for block in range(grad.shape[0] // STORE_ROWS):
        here = pl.ds(block * STORE_ROWS, STORE_ROWS)
        moved = table[here, :].astype(jnp.float32) - rate * grad[here, :]
        outbuf[here, :] = moved.astype(jnp.bfloat16)
        copy = pltpu.make_async_copy(outbuf.at[here, :], out_ref.at[here, :], out_sem.at[block])
        copy.start()
        stores.append(copy)
    rms_ref[0] = norm_ref[1, 0]
    for copy in stores:
        copy.wait()


def solution(mesh):
    n_vocab, n_dp = mesh.shape["vocab"], mesh.shape["dp"]
    n = n_vocab * n_dp

    def body(embed_table, token_ids, grad_rows):
        rows, width = embed_table.shape
        tokens = token_ids.shape[1]
        half = width // n_dp
        chunks = half // COLS
        in_vmem = pl.BlockSpec(memory_space=pltpu.VMEM)
        in_hbm = pl.BlockSpec(memory_space=pltpu.HBM)
        grad, table, norm = pl.pallas_call(
            functools.partial(kernel, (n_vocab, n_dp)),
            name="clipped_update",
            out_shape=(
                jax.ShapeDtypeStruct((rows, half), jnp.float32),
                jax.ShapeDtypeStruct((rows, half), jnp.bfloat16),
                jax.ShapeDtypeStruct((8, 128), jnp.float32),
            ),
            in_specs=[in_hbm, in_hbm, in_hbm],
            out_specs=(in_vmem, in_vmem, in_vmem),
            scratch_shapes=[
                pltpu.VMEM((n_dp * tokens, half), jnp.bfloat16),
                pltpu.VMEM((2, n_dp, TOK_EDGE, half), jnp.bfloat16),
                pltpu.VMEM((1, tokens), jnp.int32),
                pltpu.VMEM((1, tokens), jnp.int32),
                pltpu.VMEM((2, n_dp, 1, TOK_EDGE), jnp.int32),
                pltpu.VMEM((8, COLS), jnp.float32),
                pltpu.VMEM((n, 1, 128), jnp.float32),
                pltpu.SemaphoreType.DMA,
                pltpu.SemaphoreType.DMA,
                pltpu.SemaphoreType.DMA,
                pltpu.SemaphoreType.DMA((2, chunks)),
                pltpu.SemaphoreType.DMA((2,)),
                pltpu.SemaphoreType.DMA((2, n_dp, chunks)),
                pltpu.SemaphoreType.DMA((2, n_dp, chunks)),
                pltpu.SemaphoreType.DMA((2, n_dp)),
                pltpu.SemaphoreType.DMA((2, n_dp)),
                pltpu.SemaphoreType.DMA((n,)),
                pltpu.SemaphoreType.DMA((n,)),
            ],
            compiler_params=pltpu.CompilerParams(
                collective_id=0, has_side_effects=True, vmem_limit_bytes=38 * 1024 * 1024
            ),
        )(*(pltpu.with_memory_space_constraint(x, pltpu.HBM) for x in (embed_table, token_ids, grad_rows)))
        updated, grad_rms = pl.pallas_call(
            update,
            name="clipped_step",
            out_shape=(
                jax.ShapeDtypeStruct((rows, half), jnp.bfloat16),
                jax.ShapeDtypeStruct((1,), jnp.float32),
            ),
            in_specs=[in_vmem, in_vmem, in_vmem],
            out_specs=(in_hbm, pl.BlockSpec(memory_space=pltpu.SMEM)),
            scratch_shapes=[
                pltpu.VMEM((rows, half), jnp.bfloat16),
                pltpu.SemaphoreType.DMA((rows // STORE_ROWS,)),
            ],
            compiler_params=pltpu.CompilerParams(vmem_limit_bytes=24 * 1024 * 1024),
        )(grad, table, norm)
        return updated, grad_rms

    in_specs = (P("vocab", None), P("dp", "vocab"), P("dp", "vocab", None))
    out_specs = (P("vocab", "dp"), P())
    return jax.shard_map(body, mesh=mesh, in_specs=in_specs, out_specs=out_specs, check_vma=False)
```

```python
import functools

import jax
import jax.numpy as jnp
from jax import lax
from jax.experimental import pallas as pl
from jax.experimental.pallas import tpu as pltpu
from jax.sharding import PartitionSpec as P

MESH = pl.DeviceIdType.MESH
TOK_EDGE = 128
EDGE = 256
COLS = 512
STORE_ROWS = 128

step_rate = 0.5
norm_limit = 1.0


def kernel(sizes, table_ref, ids_ref, grad_ref, grad, table, norm_ref,
           toks, halo, own_ids, mate_ids, halo_ids, square, sums,
           own_sem, own_id_sem, table_sem, mate_sem, mate_id_sem, halo_send, halo_recv,
           halo_id_send, halo_id_recv, sum_send, sum_recv, known_sem):
    n_vocab, n_dp = sizes
    rows, width = table_ref.shape
    tokens = ids_ref.shape[1]
    half = width // n_dp
    n = n_vocab * n_dp
    chunks = half // COLS
    blocks = rows // EDGE
    v = lax.axis_index("vocab")
    p = lax.axis_index("dp")
    me = v * n_dp + p
    mate = 1 - p
    below = lax.rem(v + n_vocab - 1, n_vocab)
    above = lax.rem(v + 1, n_vocab)

    def columns(core, chunk):
        return pl.ds(pl.multiple_of(core * half + chunk * COLS, COLS), COLS)

    def around(distance):
        ahead = v + distance
        return jnp.where(ahead >= n_vocab, ahead - n_vocab, ahead)

    own_half = pl.ds(pl.multiple_of(p * half, half), half)
    own_copy = pltpu.make_async_copy(
        grad_ref.at[0, :, own_half], toks.at[pl.ds(0, tokens), :], own_sem
    )
    own_copy.start()
    own_id_copy = pltpu.make_async_copy(ids_ref, own_ids, own_id_sem)
    own_id_copy.start()
    table_copy = pltpu.make_async_copy(table_ref.at[:, own_half], table, table_sem)

    barrier = pltpu.get_barrier_semaphore()

    greeted = [(v, mate)] + [(w, core) for w in (below, above) for core in range(n_dp)]
    for w, core in greeted:
        pl.semaphore_signal(
            barrier, inc=1, device_id={"vocab": w, "dp": core}, device_id_type=MESH
        )
    pl.semaphore_wait(barrier, len(greeted))

    def remote(src, dst, send, recv, device):
        return pltpu.make_async_remote_copy(
            src_ref=src, dst_ref=dst, send_sem=send, recv_sem=recv,
            device_id=device, device_id_type=MESH,
        )

    sent = []
    mate_id_copy = remote(
        ids_ref, mate_ids, mate_id_sem.at[0], mate_id_sem.at[1], {"vocab": v, "dp": mate}
    )
    mate_id_copy.start()
    sides = ((0, 0, below), (1, tokens - TOK_EDGE, above))
    for side, first, target in sides:
        for core in range(n_dp):
            copy = remote(
                ids_ref.at[:, pl.ds(first, TOK_EDGE)], halo_ids.at[side, p],
                halo_id_send.at[side, core], halo_id_recv.at[side, p],
                {"vocab": target, "dp": core},
            )
            copy.start()
            sent.append(copy)
    mate_copies = []
    for chunk in range(chunks):
        for side, first, target in sides:
            for core in range(n_dp):
                copy = remote(
                    grad_ref.at[0, pl.ds(first, TOK_EDGE), columns(core, chunk)],
                    halo.at[side, p, :, pl.ds(chunk * COLS, COLS)],
                    halo_send.at[side, core, chunk], halo_recv.at[side, p, chunk],
                    {"vocab": target, "dp": core},
                )
                copy.start()
                sent.append(copy)
        copy = remote(
            grad_ref.at[0, :, columns(mate, chunk)],
            toks.at[pl.ds(tokens, tokens), pl.ds(chunk * COLS, COLS)],
            mate_sem.at[0, chunk], mate_sem.at[1, chunk], {"vocab": v, "dp": mate},
        )
        copy.start()
        mate_copies.append(copy)
    table_copy.start()

    own_start = v * rows

    def local(ids):
        shifted = ids - own_start
        return jnp.where(shifted < 0, shifted + n_vocab * rows, shifted)

    def onehot(ids, base, count):
        index = lax.broadcasted_iota(jnp.int32, (count, ids.shape[1]), 0) + base
        return jnp.where(ids == index, 1.0, 0.0).astype(jnp.bfloat16)

    def add_squares(values):
        lanes = values * values
        lanes = jnp.sum(lanes.reshape(EDGE // 8, 8, COLS), axis=0)
        square[...] += lanes

    square[...] = jnp.zeros_like(square)
    own_copy.wait()
    own_id_copy.wait()
    mate_id_copy.wait()
    for copy in mate_copies:
        copy.wait()
    rounds = []
    while 2 ** len(rounds) < n_vocab // 2:
        rounds.append(2 ** len(rounds))

    def tell(k):
        for distance in (rounds[k], n_vocab - rounds[k]):
            pl.semaphore_signal(
                known_sem.at[k], inc=1,
                device_id={"vocab": around(distance), "dp": p}, device_id_type=MESH,
            )

    window_ids = local(jnp.concatenate([own_ids[...], mate_ids[...]], axis=1))
    for block in range(blocks):
        if block < len(rounds):
            tell(block)
        picked = onehot(window_ids, block * EDGE, EDGE)

        @pl.loop(0, chunks)
        def _(chunk):
            here = pl.ds(pl.multiple_of(chunk * COLS, COLS), COLS)
            part = jnp.dot(picked, toks[:, here], preferred_element_type=jnp.float32)
            grad[pl.ds(block * EDGE, EDGE), here] = part
            if 0 < block < blocks - 1:
                add_squares(part)

        if block < len(rounds):
            pl.semaphore_wait(known_sem.at[block], 2)

    for k in range(blocks, len(rounds)):
        tell(k)
        pl.semaphore_wait(known_sem.at[k], 2)

    table_copy.wait()
    halo_pick = []
    for side in range(2):
        for core in range(n_dp):
            remote(
                ids_ref.at[:, pl.ds(0, TOK_EDGE)], halo_ids.at[side, core],
                halo_id_send.at[side, core], halo_id_recv.at[side, core],
                {"vocab": above, "dp": core},
            ).wait_recv()
        ids = local(jnp.concatenate([halo_ids[side, core] for core in range(n_dp)], axis=1))
        base = (rows - EDGE) if side == 0 else 0
        halo_pick.append((base, onehot(ids, base, EDGE)))
    for chunk in range(chunks):
        here = pl.ds(chunk * COLS, COLS)
        for side in range(2):
            for core in range(n_dp):
                remote(
                    grad_ref.at[0, pl.ds(0, TOK_EDGE), pl.ds(0, COLS)],
                    halo.at[side, core, :, here],
                    halo_send.at[side, core, chunk], halo_recv.at[side, core, chunk],
                    {"vocab": above, "dp": core},
                ).wait_recv()
            base, pick = halo_pick[side]
            part = jnp.dot(
                pick, halo[side, :, :, here].reshape(n_dp * TOK_EDGE, COLS),
                preferred_element_type=jnp.float32,
            )
            total = grad[pl.ds(base, EDGE), here] + part
            grad[pl.ds(base, EDGE), here] = total
            add_squares(total)

    lanes = jnp.sum(square[...], axis=0, keepdims=True)
    lanes = functools.reduce(
        jnp.add, [lanes[:, k * 128:(k + 1) * 128] for k in range(COLS // 128)]
    )
    sums[me] = lanes

    def sum_copy(source, slot, target):
        w, core = target
        return remote(
            sums.at[source], sums.at[source], sum_send.at[slot], sum_recv.at[source],
            {"vocab": w, "dp": core},
        )

    @pl.loop(1, n_vocab)
    def _(distance):
        for core in range(n_dp):
            sum_copy(me, distance * n_dp + core, (around(distance), core)).start()

    sum_copy(me, 0, (v, mate)).start()

    for copy in sent:
        copy.wait_send()

    sum_copy(v * n_dp + mate, 0, (v, mate)).wait_recv()

    @pl.loop(1, n_vocab)
    def _(distance):
        w = around(distance)
        for core in range(n_dp):
            sum_copy(w * n_dp + core, 0, (w, core)).wait_recv()

    total = jnp.sum(jnp.sum(sums[...], axis=0), axis=1, keepdims=True)
    rms = jnp.sqrt(total / (n_vocab * rows * width))
    clip_scale = 1.0 / jnp.maximum(1.0, rms / norm_limit)
    norm_ref[0:1, :] = jnp.broadcast_to(step_rate * clip_scale, (1, 128))
    norm_ref[1:2, :] = jnp.broadcast_to(rms, (1, 128))

    sum_copy(me, 0, (v, mate)).wait_send()

    @pl.loop(1, n_vocab)
    def _(distance):
        for core in range(n_dp):
            sum_copy(me, distance * n_dp + core, (around(distance), core)).wait_send()


def update(grad, table, norm_ref, out_ref, rms_ref, outbuf, out_sem):
    rate = norm_ref[0:1, 0:1]
    stores = []
    for block in range(grad.shape[0] // STORE_ROWS):
        here = pl.ds(block * STORE_ROWS, STORE_ROWS)
        moved = table[here, :].astype(jnp.float32) - rate * grad[here, :]
        outbuf[here, :] = moved.astype(jnp.bfloat16)
        copy = pltpu.make_async_copy(outbuf.at[here, :], out_ref.at[here, :], out_sem.at[block])
        copy.start()
        stores.append(copy)
    rms_ref[0] = norm_ref[1, 0]
    for copy in stores:
        copy.wait()


def solution(mesh):
    n_vocab, n_dp = mesh.shape["vocab"], mesh.shape["dp"]
    n = n_vocab * n_dp

    def body(embed_table, token_ids, grad_rows):
        rows, width = embed_table.shape
        tokens = token_ids.shape[1]
        half = width // n_dp
        chunks = half // COLS
        in_vmem = pl.BlockSpec(memory_space=pltpu.VMEM)
        in_hbm = pl.BlockSpec(memory_space=pltpu.HBM)
        grad, table, norm = pl.pallas_call(
            functools.partial(kernel, (n_vocab, n_dp)),
            name="clipped_update",
            out_shape=(
                jax.ShapeDtypeStruct((rows, half), jnp.float32),
                jax.ShapeDtypeStruct((rows, half), jnp.bfloat16),
                jax.ShapeDtypeStruct((8, 128), jnp.float32),
            ),
            in_specs=[in_hbm, in_hbm, in_hbm],
            out_specs=(in_vmem, in_vmem, in_vmem),
            scratch_shapes=[
                pltpu.VMEM((n_dp * tokens, half), jnp.bfloat16),
                pltpu.VMEM((2, n_dp, TOK_EDGE, half), jnp.bfloat16),
                pltpu.VMEM((1, tokens), jnp.int32),
                pltpu.VMEM((1, tokens), jnp.int32),
                pltpu.VMEM((2, n_dp, 1, TOK_EDGE), jnp.int32),
                pltpu.VMEM((8, COLS), jnp.float32),
                pltpu.VMEM((n, 1, 128), jnp.float32),
                pltpu.SemaphoreType.DMA,
                pltpu.SemaphoreType.DMA,
                pltpu.SemaphoreType.DMA,
                pltpu.SemaphoreType.DMA((2, chunks)),
                pltpu.SemaphoreType.DMA((2,)),
                pltpu.SemaphoreType.DMA((2, n_dp, chunks)),
                pltpu.SemaphoreType.DMA((2, n_dp, chunks)),
                pltpu.SemaphoreType.DMA((2, n_dp)),
                pltpu.SemaphoreType.DMA((2, n_dp)),
                pltpu.SemaphoreType.DMA((n,)),
                pltpu.SemaphoreType.DMA((n,)),
                pltpu.SemaphoreType.REGULAR((max(n_vocab.bit_length(), 1),)),
            ],
            compiler_params=pltpu.CompilerParams(
                collective_id=0, has_side_effects=True, vmem_limit_bytes=38 * 1024 * 1024
            ),
        )(*(pltpu.with_memory_space_constraint(x, pltpu.HBM) for x in (embed_table, token_ids, grad_rows)))
        updated, grad_rms = pl.pallas_call(
            update,
            name="clipped_step",
            out_shape=(
                jax.ShapeDtypeStruct((rows, half), jnp.bfloat16),
                jax.ShapeDtypeStruct((1,), jnp.float32),
            ),
            in_specs=[in_vmem, in_vmem, in_vmem],
            out_specs=(in_hbm, pl.BlockSpec(memory_space=pltpu.SMEM)),
            scratch_shapes=[
                pltpu.VMEM((rows, half), jnp.bfloat16),
                pltpu.SemaphoreType.DMA((rows // STORE_ROWS,)),
            ],
            compiler_params=pltpu.CompilerParams(vmem_limit_bytes=24 * 1024 * 1024),
        )(grad, table, norm)
        return updated, grad_rms

    in_specs = (P("vocab", None), P("dp", "vocab"), P("dp", "vocab", None))
    out_specs = (P("vocab", "dp"), P())
    return jax.shard_map(body, mesh=mesh, in_specs=in_specs, out_specs=out_specs, check_vma=False)
```

```python
import functools

import jax
import jax.numpy as jnp
from jax import lax
from jax.experimental import pallas as pl
from jax.experimental.pallas import tpu as pltpu
from jax.sharding import PartitionSpec as P

MESH = pl.DeviceIdType.MESH
TOK_EDGE = 128
EDGE = 256
COLS = 512
STORE_ROWS = 64

step_rate = 0.5
norm_limit = 1.0


def kernel(sizes, table_ref, ids_ref, grad_ref, grad, table, norm_ref,
           toks, halo, own_ids, mate_ids, halo_ids, square, sums,
           own_sem, own_id_sem, table_sem, mate_sem, mate_id_sem, halo_send, halo_recv,
           halo_id_send, halo_id_recv, sum_send, sum_recv, known_sem):
    n_vocab, n_dp = sizes
    rows, width = table_ref.shape
    tokens = ids_ref.shape[1]
    half = width // n_dp
    n = n_vocab * n_dp
    chunks = half // COLS
    blocks = rows // EDGE
    v = lax.axis_index("vocab")
    p = lax.axis_index("dp")
    me = v * n_dp + p
    mate = 1 - p
    below = lax.rem(v + n_vocab - 1, n_vocab)
    above = lax.rem(v + 1, n_vocab)

    def columns(core, chunk):
        return pl.ds(pl.multiple_of(core * half + chunk * COLS, COLS), COLS)

    def around(distance):
        ahead = v + distance
        return jnp.where(ahead >= n_vocab, ahead - n_vocab, ahead)

    own_half = pl.ds(pl.multiple_of(p * half, half), half)
    own_copy = pltpu.make_async_copy(
        grad_ref.at[0, :, own_half], toks.at[pl.ds(0, tokens), :], own_sem
    )
    own_copy.start()
    own_id_copy = pltpu.make_async_copy(ids_ref, own_ids, own_id_sem)
    own_id_copy.start()
    table_copy = pltpu.make_async_copy(table_ref.at[:, own_half], table, table_sem)

    barrier = pltpu.get_barrier_semaphore()

    greeted = [(v, mate)] + [(w, core) for w in (below, above) for core in range(n_dp)]
    for w, core in greeted:
        pl.semaphore_signal(
            barrier, inc=1, device_id={"vocab": w, "dp": core}, device_id_type=MESH
        )
    pl.semaphore_wait(barrier, len(greeted))

    def remote(src, dst, send, recv, device):
        return pltpu.make_async_remote_copy(
            src_ref=src, dst_ref=dst, send_sem=send, recv_sem=recv,
            device_id=device, device_id_type=MESH,
        )

    sent = []
    mate_id_copy = remote(
        ids_ref, mate_ids, mate_id_sem.at[0], mate_id_sem.at[1], {"vocab": v, "dp": mate}
    )
    mate_id_copy.start()
    sides = ((0, 0, below), (1, tokens - TOK_EDGE, above))
    for side, first, target in sides:
        for core in range(n_dp):
            copy = remote(
                ids_ref.at[:, pl.ds(first, TOK_EDGE)], halo_ids.at[side, p],
                halo_id_send.at[side, core], halo_id_recv.at[side, p],
                {"vocab": target, "dp": core},
            )
            copy.start()
            sent.append(copy)
    mate_copies = []
    for chunk in range(chunks):
        for side, first, target in sides:
            for core in range(n_dp):
                copy = remote(
                    grad_ref.at[0, pl.ds(first, TOK_EDGE), columns(core, chunk)],
                    halo.at[side, p, :, pl.ds(chunk * COLS, COLS)],
                    halo_send.at[side, core, chunk], halo_recv.at[side, p, chunk],
                    {"vocab": target, "dp": core},
                )
                copy.start()
                sent.append(copy)
        copy = remote(
            grad_ref.at[0, :, columns(mate, chunk)],
            toks.at[pl.ds(tokens, tokens), pl.ds(chunk * COLS, COLS)],
            mate_sem.at[0, chunk], mate_sem.at[1, chunk], {"vocab": v, "dp": mate},
        )
        copy.start()
        mate_copies.append(copy)
    table_copy.start()

    own_start = v * rows

    def local(ids):
        shifted = ids - own_start
        return jnp.where(shifted < 0, shifted + n_vocab * rows, shifted)

    def onehot(ids, base, count):
        index = lax.broadcasted_iota(jnp.int32, (count, ids.shape[1]), 0) + base
        return jnp.where(ids == index, 1.0, 0.0).astype(jnp.bfloat16)

    def add_squares(values):
        lanes = values * values
        lanes = jnp.sum(lanes.reshape(EDGE // 8, 8, COLS), axis=0)
        square[...] += lanes

    square[...] = jnp.zeros_like(square)
    own_copy.wait()
    own_id_copy.wait()
    mate_id_copy.wait()
    for copy in mate_copies:
        copy.wait()
    rounds = []
    while 2 ** len(rounds) < n_vocab // 2:
        rounds.append(2 ** len(rounds))

    def tell(k):
        for distance in (rounds[k], n_vocab - rounds[k]):
            pl.semaphore_signal(
                known_sem.at[k], inc=1,
                device_id={"vocab": around(distance), "dp": p}, device_id_type=MESH,
            )

    window_ids = local(jnp.concatenate([own_ids[...], mate_ids[...]], axis=1))
    for block in range(blocks):
        if block < len(rounds):
            tell(block)
        picked = onehot(window_ids, block * EDGE, EDGE)

        @pl.loop(0, chunks)
        def _(chunk):
            here = pl.ds(pl.multiple_of(chunk * COLS, COLS), COLS)
            part = jnp.dot(picked, toks[:, here], preferred_element_type=jnp.float32)
            grad[pl.ds(block * EDGE, EDGE), here] = part
            if 0 < block < blocks - 1:
                add_squares(part)

        if block < len(rounds):
            pl.semaphore_wait(known_sem.at[block], 2)

    for k in range(blocks, len(rounds)):
        tell(k)
        pl.semaphore_wait(known_sem.at[k], 2)

    table_copy.wait()
    halo_pick = []
    for side in range(2):
        for core in range(n_dp):
            remote(
                ids_ref.at[:, pl.ds(0, TOK_EDGE)], halo_ids.at[side, core],
                halo_id_send.at[side, core], halo_id_recv.at[side, core],
                {"vocab": above, "dp": core},
            ).wait_recv()
        ids = local(jnp.concatenate([halo_ids[side, core] for core in range(n_dp)], axis=1))
        base = (rows - EDGE) if side == 0 else 0
        halo_pick.append((base, onehot(ids, base, EDGE)))
    for chunk in range(chunks):
        here = pl.ds(chunk * COLS, COLS)
        for side in range(2):
            for core in range(n_dp):
                remote(
                    grad_ref.at[0, pl.ds(0, TOK_EDGE), pl.ds(0, COLS)],
                    halo.at[side, core, :, here],
                    halo_send.at[side, core, chunk], halo_recv.at[side, core, chunk],
                    {"vocab": above, "dp": core},
                ).wait_recv()
            base, pick = halo_pick[side]
            part = jnp.dot(
                pick, halo[side, :, :, here].reshape(n_dp * TOK_EDGE, COLS),
                preferred_element_type=jnp.float32,
            )
            total = grad[pl.ds(base, EDGE), here] + part
            grad[pl.ds(base, EDGE), here] = total
            add_squares(total)

    lanes = jnp.sum(square[...], axis=0, keepdims=True)
    lanes = functools.reduce(
        jnp.add, [lanes[:, k * 128:(k + 1) * 128] for k in range(COLS // 128)]
    )
    sums[me] = lanes

    def sum_copy(source, slot, target):
        w, core = target
        return remote(
            sums.at[source], sums.at[source], sum_send.at[slot], sum_recv.at[source],
            {"vocab": w, "dp": core},
        )

    @pl.loop(1, n_vocab)
    def _(distance):
        for core in range(n_dp):
            sum_copy(me, distance * n_dp + core, (around(distance), core)).start()

    sum_copy(me, 0, (v, mate)).start()

    for copy in sent:
        copy.wait_send()

    sum_copy(v * n_dp + mate, 0, (v, mate)).wait_recv()

    @pl.loop(1, n_vocab)
    def _(distance):
        w = around(distance)
        for core in range(n_dp):
            sum_copy(w * n_dp + core, 0, (w, core)).wait_recv()

    total = jnp.sum(jnp.sum(sums[...], axis=0), axis=1, keepdims=True)
    rms = jnp.sqrt(total / (n_vocab * rows * width))
    clip_scale = 1.0 / jnp.maximum(1.0, rms / norm_limit)
    norm_ref[0:1, :] = jnp.broadcast_to(step_rate * clip_scale, (1, 128))
    norm_ref[1:2, :] = jnp.broadcast_to(rms, (1, 128))

    sum_copy(me, 0, (v, mate)).wait_send()

    @pl.loop(1, n_vocab)
    def _(distance):
        for core in range(n_dp):
            sum_copy(me, distance * n_dp + core, (around(distance), core)).wait_send()


def update(grad, table, norm_ref, out_ref, rms_ref, outbuf, rms_held, out_sem, rms_sem):
    rms_held[0] = norm_ref[1, 0]
    rms_copy = pltpu.make_async_copy(rms_held, rms_ref, rms_sem)
    rms_copy.start()
    rate = norm_ref[0:1, 0:1]
    stores = []
    for block in range(grad.shape[0] // STORE_ROWS):
        here = pl.ds(block * STORE_ROWS, STORE_ROWS)
        moved = table[here, :].astype(jnp.float32) - rate * grad[here, :]
        outbuf[here, :] = moved.astype(jnp.bfloat16)
        copy = pltpu.make_async_copy(outbuf.at[here, :], out_ref.at[here, :], out_sem.at[block])
        copy.start()
        stores.append(copy)
    for copy in stores:
        copy.wait()
    rms_copy.wait()


def solution(mesh):
    n_vocab, n_dp = mesh.shape["vocab"], mesh.shape["dp"]
    n = n_vocab * n_dp

    def body(embed_table, token_ids, grad_rows):
        rows, width = embed_table.shape
        tokens = token_ids.shape[1]
        half = width // n_dp
        chunks = half // COLS
        in_vmem = pl.BlockSpec(memory_space=pltpu.VMEM)
        in_hbm = pl.BlockSpec(memory_space=pltpu.HBM)
        grad, table, norm = pl.pallas_call(
            functools.partial(kernel, (n_vocab, n_dp)),
            name="clipped_update",
            out_shape=(
                jax.ShapeDtypeStruct((rows, half), jnp.float32),
                jax.ShapeDtypeStruct((rows, half), jnp.bfloat16),
                jax.ShapeDtypeStruct((8, 128), jnp.float32),
            ),
            in_specs=[in_hbm, in_hbm, in_hbm],
            out_specs=(in_vmem, in_vmem, in_vmem),
            scratch_shapes=[
                pltpu.VMEM((n_dp * tokens, half), jnp.bfloat16),
                pltpu.VMEM((2, n_dp, TOK_EDGE, half), jnp.bfloat16),
                pltpu.VMEM((1, tokens), jnp.int32),
                pltpu.VMEM((1, tokens), jnp.int32),
                pltpu.VMEM((2, n_dp, 1, TOK_EDGE), jnp.int32),
                pltpu.VMEM((8, COLS), jnp.float32),
                pltpu.VMEM((n, 1, 128), jnp.float32),
                pltpu.SemaphoreType.DMA,
                pltpu.SemaphoreType.DMA,
                pltpu.SemaphoreType.DMA,
                pltpu.SemaphoreType.DMA((2, chunks)),
                pltpu.SemaphoreType.DMA((2,)),
                pltpu.SemaphoreType.DMA((2, n_dp, chunks)),
                pltpu.SemaphoreType.DMA((2, n_dp, chunks)),
                pltpu.SemaphoreType.DMA((2, n_dp)),
                pltpu.SemaphoreType.DMA((2, n_dp)),
                pltpu.SemaphoreType.DMA((n,)),
                pltpu.SemaphoreType.DMA((n,)),
                pltpu.SemaphoreType.REGULAR((max(n_vocab.bit_length(), 1),)),
            ],
            compiler_params=pltpu.CompilerParams(
                collective_id=0, has_side_effects=True, vmem_limit_bytes=38 * 1024 * 1024
            ),
        )(*(pltpu.with_memory_space_constraint(x, pltpu.HBM) for x in (embed_table, token_ids, grad_rows)))
        updated, grad_rms = pl.pallas_call(
            update,
            name="clipped_step",
            out_shape=(
                jax.ShapeDtypeStruct((rows, half), jnp.bfloat16),
                jax.ShapeDtypeStruct((1,), jnp.float32),
            ),
            in_specs=[in_vmem, in_vmem, in_vmem],
            out_specs=(in_hbm, in_hbm),
            scratch_shapes=[
                pltpu.VMEM((rows, half), jnp.bfloat16),
                pltpu.SMEM((1,), jnp.float32),
                pltpu.SemaphoreType.DMA((rows // STORE_ROWS,)),
                pltpu.SemaphoreType.DMA,
            ],
            compiler_params=pltpu.CompilerParams(vmem_limit_bytes=24 * 1024 * 1024),
        )(grad, table, norm)
        return updated, grad_rms

    in_specs = (P("vocab", None), P("dp", "vocab"), P("dp", "vocab", None))
    out_specs = (P("vocab", "dp"), P())
    return jax.shard_map(body, mesh=mesh, in_specs=in_specs, out_specs=out_specs, check_vma=False)
```
